32 devices in a mesh: shot: 2 (over y), gx: 4 (over z), gy: 4 (over x, core).
Axes of the slice: x: 2, y: 2, z: 4, core: 2. Of those that a mesh axis runs over, the one named last changes fastest.
Arguments:
- wavefield: float32 [9, 64, 64, 128], P(None, ('shot', 'gx'), 'gy'), parts along dimension 1, may hold values from -10 to 10
- labels: int32 [32, 64, 128], P('gx', 'gy'), may hold values from 0 to 7
- lame_table: float32 [8], replicated, may hold values from 0.5 to 2
- shear_table: float32 [8], replicated, may hold values from 0.1 to 0.6
- density_table: float32 [8], replicated, may hold values from 0.8 to 2
- source_cells: int32 [128], P('shot'), parts along dimension 0, may hold values from 0 to 262143
- source_amps: float32 [5, 128], P(None, 'shot'), parts along dimension 1, may hold values from -6 to 6
- receiver_cells: int32 [256], replicated, may hold values from 0 to 262143
Outputs:
- final_fields: float32 [9, 64, 64, 128], P(None, ('shot', 'gx'), 'gy'), parts along dimension 1
- traces: float32 [5, 512], P(None, 'shot'), parts along dimension 1
The draws below stay inside these ranges and needn't reach their ends.
There are 2 independent parts, one for each index of `shot`. The reference program is written for one: setup_inputs(seed, part) draws one part's arguments, and reference() takes and returns one part's arrays. A program takes and returns all parts, laid end to end along the dimension named above; an argument that names none is the same for every part. Nothing has to cross between parts.
Inputs may be any that keep to these rules, and one draw needn't show every extreme that they name: `source_cells`: a flat cell index, x slowest, z fastest. `receiver_cells`: a flat cell index, x slowest, z fastest.
All inputs are finite; a program needn't handle non-finite values.
Results may differ from the reference program's by a relative error of at most 0.00002.
Values sent between devices are 32-bit elements; how exact they have to be, the bound alone decides.
A program may use at most 64 MiB of HBM per device.

```python
import math
import jax
import jax.numpy as jnp

NZ = 128
STEPS = 5
NLAB = 8
NSRC = 64
NREC = 256
NX = 32
NY = 64


def smooth_modes(key, count, amp_lo, amp_hi, wave_lo, wave_hi):
    keys = jax.random.split(key, 4)
    lengths = jax.random.uniform(keys[0], (3, count, 3), jnp.float32, wave_lo, wave_hi)
    flips = jax.random.uniform(keys[1], (3, count, 3), jnp.float32)
    signs = jnp.where(flips < 0.5, -1.0, 1.0).astype(jnp.float32)
    waves = signs * (2.0 * math.pi) / lengths
    phases = jax.random.uniform(keys[2], (3, count), jnp.float32, 0.0, 2.0 * math.pi)
    amps = jax.random.uniform(keys[3], (3, count), jnp.float32, amp_lo, amp_hi)
    coord_x = jnp.arange(NX, dtype=jnp.float32)[:, None, None]
    coord_y = jnp.arange(NY, dtype=jnp.float32)[None, :, None]
    coord_z = jnp.arange(NZ, dtype=jnp.float32)[None, None, :]
    components = []
    for comp in range(3):
        total = jnp.zeros((NX, NY, NZ), jnp.float32)
        for mode in range(count):
            angle = waves[comp, mode, 0] * coord_x + waves[comp, mode, 1] * coord_y + waves[comp, mode, 2] * coord_z + phases[comp, mode]
            total = total + amps[comp, mode] * jnp.cos(angle)
        components.append(total)
    return jnp.stack(components)


def draw_wavefield(key, part):
    key_modes = jax.random.fold_in(key, 11)
    key_rough = jax.random.fold_in(key, 12)
    key_stress = jax.random.fold_in(key, 13)
    smooth = smooth_modes(key_modes, 4, 1.2, 1.8, 16.0, 48.0)
    rough = 0.2 * jnp.clip(jax.random.normal(key_rough, (3, NX, NY, NZ), jnp.float32), -6.0, 6.0)
    stress = 0.25 * jnp.clip(jax.random.normal(key_stress, (6, NX, NY, NZ), jnp.float32), -6.0, 6.0)
    return jnp.concatenate([smooth + rough, stress], axis=0).astype(jnp.float32)


def place_ends(array, rng, low, largest):
    shape = array.shape
    place = [jax.random.randint(jax.random.fold_in(rng, axis), (), 0, shape[axis]) for axis in range(len(shape))]
    array = array.at[tuple(place)].set(low)
    longest = shape.index(max(shape))
    place[longest] = (place[longest] + 1) % shape[longest]
    return array.at[tuple(place)].set(largest)


def normal_values(own_key, shape, spread, most, kind=jnp.bfloat16):
    return jnp.clip(spread * jax.random.normal(own_key, shape, jnp.float32), -most, most).astype(kind)


def setup_inputs(seed: int = 0, part: int = 0) -> dict:
    splits = jax.random.split(jax.random.key(seed), 9)
    part_splits = jax.random.split(jax.random.fold_in(splits[8], part), 9)
    return {
        "wavefield": draw_wavefield(jax.random.fold_in(jax.random.fold_in(splits[8], part), 71), part),
        "labels": place_ends(jax.random.randint(splits[1], (NX, NY, NZ), 0, NLAB), jax.random.fold_in(splits[1], 1), 0, NLAB - 1).astype(jnp.int32),
        "lame_table": jnp.clip(jnp.exp(jax.random.uniform(splits[2], (NLAB,), jnp.float32, math.log(0.5), math.log(2.0))), 0.5, 2.0),
        "shear_table": jnp.clip(jnp.exp(jax.random.uniform(splits[3], (NLAB,), jnp.float32, math.log(0.1), math.log(0.6))), 0.1, 0.6),
        "density_table": jnp.clip(jnp.exp(jax.random.uniform(splits[4], (NLAB,), jnp.float32, math.log(0.8), math.log(2.0))), 0.8, 2.0),
        "source_cells": place_ends(jax.random.randint(part_splits[5], (NSRC,), 0, NX * NY * NZ), jax.random.fold_in(part_splits[5], 1), 0, (NX * NY * NZ) - 1).astype(jnp.int32),
        "source_amps": normal_values(part_splits[6], (STEPS, NSRC), 1.0, 6.0, jnp.float32),
        "receiver_cells": place_ends(jax.random.randint(splits[7], (NREC,), 0, NX * NY * NZ), jax.random.fold_in(splits[7], 1), 0, (NX * NY * NZ) - 1).astype(jnp.int32),
    }


stencil_coeffs = (1225.0 / 1024.0, -245.0 / 3072.0, 49.0 / 5120.0, -5.0 / 7168.0)
time_step = 0.15
sponge_width = 16.0


def shifted(padded, offset, direction, layout):
    padding, margins, extent = layout
    pieces = []
    for dimension in range(3):
        start = padding[dimension] - margins[dimension] + (offset if dimension == direction else 0)
        pieces.append(slice(start, start + extent[dimension] + 2 * margins[dimension]))
    return padded[tuple(pieces)]


def derivative(padded, direction, forward, layout):
    result = None
    for number in range(1, 5):
        if forward:
            later, earlier = number, 1 - number
        else:
            later, earlier = number - 1, -number
        term = stencil_coeffs[number - 1] * (shifted(padded, later, direction, layout) - shifted(padded, earlier, direction, layout))
        result = term if result is None else result + term
    return result


def velocity_update(velocity, stress_padded, buoyancy, layout):
    normal_x, normal_y, normal_z = stress_padded[0], stress_padded[1], stress_padded[2]
    shear_xy, shear_xz, shear_yz = stress_padded[3], stress_padded[4], stress_padded[5]
    velocity_x = velocity[0] + time_step * buoyancy * (derivative(normal_x, 0, True, layout) + derivative(shear_xy, 1, False, layout) + derivative(shear_xz, 2, False, layout))
    velocity_y = velocity[1] + time_step * buoyancy * (derivative(shear_xy, 0, False, layout) + derivative(normal_y, 1, True, layout) + derivative(shear_yz, 2, False, layout))
    velocity_z = velocity[2] + time_step * buoyancy * (derivative(shear_xz, 0, False, layout) + derivative(shear_yz, 1, False, layout) + derivative(normal_z, 2, True, layout))
    return [velocity_x, velocity_y, velocity_z]


def stress_update(stress, velocity_padded, lame_first, shear, layout):
    velocity_x, velocity_y, velocity_z = velocity_padded[0], velocity_padded[1], velocity_padded[2]
    strain_x = derivative(velocity_x, 0, False, layout)
    strain_y = derivative(velocity_y, 1, False, layout)
    strain_z = derivative(velocity_z, 2, False, layout)
    volume = strain_x + strain_y + strain_z
    normal_x = stress[0] + time_step * (lame_first * volume + 2.0 * shear * strain_x)
    normal_y = stress[1] + time_step * (lame_first * volume + 2.0 * shear * strain_y)
    normal_z = stress[2] + time_step * (lame_first * volume + 2.0 * shear * strain_z)
    shear_xy = stress[3] + time_step * shear * (derivative(velocity_x, 1, True, layout) + derivative(velocity_y, 0, True, layout))
    shear_xz = stress[4] + time_step * shear * (derivative(velocity_x, 2, True, layout) + derivative(velocity_z, 0, True, layout))
    shear_yz = stress[5] + time_step * shear * (derivative(velocity_y, 2, True, layout) + derivative(velocity_z, 1, True, layout))
    return [normal_x, normal_y, normal_z, shear_xy, shear_xz, shear_yz]


def lookup(labels, table):
    result = jnp.zeros(labels.shape, jnp.float32)
    for label in range(table.shape[0]):
        result = result + jnp.where(labels == label, table[label], jnp.zeros((), table.dtype))
    return result


def profile(position, count):
    distance = jnp.minimum(position, count - 1 - position).astype(jnp.float32)
    depth = jnp.maximum(sponge_width - distance, 0.0) / sponge_width
    return jnp.exp(-(0.5 * depth) * (0.5 * depth))


def reference(wavefield, labels, lame_table, shear_table, density_table, source_cells, source_amps, receiver_cells):
    lame_first = lookup(labels, lame_table)
    shear = lookup(labels, shear_table)
    buoyancy = 1.0 / lookup(labels, density_table)
    damping = profile(jnp.arange(NX, dtype=jnp.int32), NX)[:, None, None] * profile(jnp.arange(NY, dtype=jnp.int32), NY)[None, :, None] * profile(jnp.arange(NZ, dtype=jnp.int32), NZ)[None, None, :]
    layout = ((4, 4, 4), (0, 0, 0), (NX, NY, NZ))
    source_x = source_cells // (NY * NZ)
    source_y = (source_cells // NZ) % NY
    source_z = source_cells % NZ
    probe_x = receiver_cells // (NY * NZ)
    probe_y = (receiver_cells // NZ) % NY
    probe_z = receiver_cells % NZ
    fields = [wavefield[number] for number in range(9)]
    rows = []
    for step in range(STEPS):
        padded_stress = [jnp.pad(field, 4) for field in fields[3:]]
        velocity = velocity_update(fields[:3], padded_stress, buoyancy, layout)
        padded_velocity = [jnp.pad(field, 4) for field in velocity]
        stress = stress_update(fields[3:], padded_velocity, lame_first, shear, layout)
        push = time_step * source_amps[step]
        for number in range(3):
            stress[number] = stress[number].at[source_x, source_y, source_z].add(push)
        fields = [field * damping for field in velocity + stress]
        pressure = -(fields[3][probe_x, probe_y, probe_z] + fields[4][probe_x, probe_y, probe_z] + fields[5][probe_x, probe_y, probe_z]) / 3.0
        rows.append(pressure)
    return jnp.stack(fields), jnp.stack(rows)
```

```python
import functools

import jax
import jax.numpy as jnp
from jax import lax
from jax.experimental import pallas as pl
from jax.experimental.pallas import tpu as pltpu
from jax.sharding import PartitionSpec as P

coeffs = (1225.0 / 1024.0, -245.0 / 3072.0, 49.0 / 5120.0, -5.0 / 7168.0)
time_step = 0.15
sponge_width = 16.0

VX, VY, VZ, SXX, SYY, SZZ, SXY, SXZ, SYZ = range(9)
EXCHANGED = {
    (SXY, 0): False, (SXX, 0): True, (SXZ, 0): False,
    (SYY, 1): True, (SXY, 1): False, (SYZ, 1): False,
    (VY, 0): True, (VX, 0): False, (VZ, 0): True,
    (VX, 1): True, (VY, 1): False, (VZ, 1): True,
}
SLOT = {key: number for number, key in enumerate(EXCHANGED)}
RIM_X = 4
RIM_Y = 8
EXACT = lax.Precision.HIGHEST


def quotient(value, count):
    if count & (count - 1) == 0:
        return lax.shift_right_logical(value, jnp.full(value.shape, count.bit_length() - 1, value.dtype))
    return lax.div(value, jnp.full(value.shape, count, value.dtype))


def remainder(value, count):
    if count & (count - 1) == 0:
        return value & (count - 1)
    return value - quotient(value, count) * count


def profile(position, count):
    distance = jnp.minimum(position, count - 1 - position).astype(jnp.float32)
    depth = jnp.maximum(sponge_width - distance, 0.0) / sponge_width
    return jnp.exp(-(0.5 * depth) * (0.5 * depth))


def kernel(
    sizes,
    wave_ref, labels_ref, lame_ref, shear_ref, density_ref,
    source_ref, amps_ref, probe_ref,
    out_ref, traces_ref,
    F, labels, lame, shear, buoy, damp, bands, source_z, probe_z, probe_row, push, press,
    rows_y, rows_x,
    load_sem, send_sem, recv_sem, tsend_y, trecv_y, tsend_x, trecv_x,
):
    nx, ny, steps = sizes
    _, wx, wy, nz = wave_ref.shape
    gx, gy = lax.axis_index("gx"), lax.axis_index("gy")
    place = (gx, gy)
    extent = (nx, ny)
    axis_name = ("gx", "gy")
    LX, LY = slice(RIM_X, RIM_X + wx), slice(RIM_Y, RIM_Y + wy)

    def local(f):
        return F.at[f, LX, LY, :]

    loads = [
        pltpu.make_async_copy(wave_ref.at[f], local(f), load_sem.at[f]) for f in range(9)
    ]
    load_labels = pltpu.make_async_copy(labels_ref, labels, load_sem.at[9])
    for f in (SXY, SXX, SXZ, SYY, SYZ):
        loads[f].start()
    load_labels.start()
    for f in (SZZ, VY, VX, VZ):
        loads[f].start()

    for f, axis in EXCHANGED:
        if axis == 0:
            F[f, :RIM_X, LY, :] = jnp.zeros((RIM_X, wy, nz), jnp.float32)
            F[f, RIM_X + wx :, LY, :] = jnp.zeros((RIM_X, wy, nz), jnp.float32)
        else:
            F[f, LX, :RIM_Y, :] = jnp.zeros((wx, RIM_Y, nz), jnp.float32)
            F[f, LX, RIM_Y + wy :, :] = jnp.zeros((wx, RIM_Y, nz), jnp.float32)
    rows_y[...] = jnp.zeros(rows_y.shape, jnp.float32)

    barrier = pltpu.get_barrier_semaphore()
    for axis in (0, 1):
        for d in range(1, extent[axis]):
            pl.semaphore_signal(
                barrier, inc=1,
                device_id={axis_name[axis]: lax.rem(place[axis] + d, extent[axis])},
                device_id_type=pl.DeviceIdType.MESH,
            )
    pl.semaphore_wait(barrier, nx + ny - 2)

    def copy(f, axis, up):
        forward = EXCHANGED[f, axis]
        n = extent[axis]
        target = lax.rem(place[axis] + (1 if up else n - 1), n)
        if axis == 0:
            count = 3 if forward == up else 4
            if up:
                src, dst = RIM_X + wx - count, RIM_X - count
            else:
                src, dst = RIM_X, RIM_X + wx
            source = F.at[f, src : src + count, LY, :]
            sink = F.at[f, dst : dst + count, LY, :]
        else:
            src, dst = (wy, 0) if up else (RIM_Y, RIM_Y + wy)
            source = F.at[f, LX, src : src + RIM_Y, :]
            sink = F.at[f, LX, dst : dst + RIM_Y, :]
        slot = SLOT[f, axis]
        return pltpu.make_async_remote_copy(
            src_ref=source, dst_ref=sink,
            send_sem=send_sem.at[slot, int(up)], recv_sem=recv_sem.at[slot, int(up)],
            device_id={axis_name[axis]: target}, device_id_type=pl.DeviceIdType.MESH,
        )

    has_low = (gx > 0, gy > 0)
    has_high = (gx < nx - 1, gy < ny - 1)

    def send(*keys):
        for f, axis in keys:
            @pl.when(has_high[axis])
            def _():
                copy(f, axis, True).start()

            @pl.when(has_low[axis])
            def _():
                copy(f, axis, False).start()

    def sent(*keys):
        for axis in (0, 1):
            mine = [f for f, a in keys if a == axis]

            @pl.when(has_high[axis])
            def _():
                for f in mine:
                    copy(f, axis, True).wait_send()

            @pl.when(has_low[axis])
            def _():
                for f in mine:
                    copy(f, axis, False).wait_send()

    def arrived(*keys):
        for f, axis in keys:
            @pl.when(has_low[axis])
            def _():
                copy(f, axis, True).wait_recv()

            @pl.when(has_high[axis])
            def _():
                copy(f, axis, False).wait_recv()

    def tap(f, axis, offset):
        if axis == 0:
            return F[f, RIM_X + offset : RIM_X + offset + wx, LY, :]
        return F[f, LX, RIM_Y + offset : RIM_Y + offset + wy, :]

    def along(f, axis):
        forward = EXCHANGED[f, axis]
        result = None
        for k in range(1, 5):
            later, earlier = (k, 1 - k) if forward else (k - 1, -k)
            term = coeffs[k - 1] * (tap(f, axis, later) - tap(f, axis, earlier))
            result = term if result is None else result + term
        return result

    def depth(f, forward):
        flat = F[f, LX, LY, :].reshape(wx * wy, nz)
        return jnp.dot(
            flat, bands[int(forward)], precision=EXACT, preferred_element_type=jnp.float32
        ).reshape(wx, wy, nz)

    stress_keys = [(SXY, 0), (SYY, 1), (SXX, 0), (SXY, 1), (SXZ, 0), (SYZ, 1)]
    speed_keys = [(VY, 0), (VX, 1), (VX, 0), (VY, 1), (VZ, 0), (VZ, 1)]

    for f in (SXY, SYY, SXX, SXZ, SYZ):
        loads[f].wait()
    send(*stress_keys)

    load_labels.wait()
    tissue = labels[...]

    def lookup(table):
        value = jnp.zeros(tissue.shape, jnp.float32)
        for number in range(table.shape[0]):
            value = jnp.where(tissue == number, table[number], value)
        return value

    lame[...] = time_step * lookup(lame_ref)
    shear[...] = time_step * lookup(shear_ref)
    buoy[...] = time_step / lookup(density_ref)
    shape = (wx, wy, nz)
    damp[...] = (
        profile(gx * wx + lax.broadcasted_iota(jnp.int32, shape, 0), nx * wx)
        * profile(gy * wy + lax.broadcasted_iota(jnp.int32, shape, 1), ny * wy)
        * profile(lax.broadcasted_iota(jnp.int32, shape, 2), nz)
    )
    gap = lax.broadcasted_iota(jnp.int32, (nz, nz), 0) - lax.broadcasted_iota(
        jnp.int32, (nz, nz), 1
    )
    for forward in (0, 1):
        band = jnp.zeros((nz, nz), jnp.float32)
        for k in range(1, 5):
            later, earlier = (k, 1 - k) if forward else (k - 1, -k)
            band = jnp.where(gap == later, coeffs[k - 1], band)
            band = jnp.where(gap == earlier, -coeffs[k - 1], band)
        bands[forward] = band

    def locate(cells):
        cell_x = quotient(cells, ny * wy * nz)
        cell_y = remainder(quotient(cells, nz), ny * wy)
        near_x = cell_x - gx * wx
        near_y = cell_y - gy * wy
        inside = (near_x >= 0) & (near_x < wx) & (near_y >= 0) & (near_y < wy)
        return jnp.where(inside, near_x * wy + near_y, -1), remainder(cells, nz)

    def match(indices, count):
        wide = (count, indices.shape[1])
        return jnp.where(lax.broadcasted_iota(jnp.int32, wide, 0) == indices, 1.0, 0.0).astype(
            jnp.float32
        )

    row, deep = locate(source_ref[...])
    source_row = match(row, wx * wy)
    source_z[...] = match(deep, nz)
    row, deep = locate(probe_ref[...])
    probe_row[...] = match(row, wx * wy)
    probe_z[...] = match(deep, nz)
    for t in range(steps):
        push[t] = lax.dot_general(
            source_row * (time_step * amps_ref[t : t + 1, :]),
            source_z[...],
            (((1,), (1,)), ((), ())),
            precision=EXACT,
            preferred_element_type=jnp.float32,
        ).reshape(wx, wy, nz)

    for f in (SZZ, VY, VX, VZ):
        loads[f].wait()

    def put(f, value):
        F[f, LX, LY, :] = value

    def get(f):
        return F[f, LX, LY, :]

    def step(t, carry):
        fade = jnp.where(t == 0, 1.0, damp[...])
        z_y = depth(SYZ, False)
        z_x = depth(SXZ, False)
        z_z = depth(SZZ, True)
        arrived((SXY, 0), (SYY, 1))
        put(VY, fade * get(VY) + buoy[...] * (along(SXY, 0) + along(SYY, 1) + z_y))
        send((VY, 0), (VY, 1))
        arrived((SXX, 0), (SXY, 1))
        put(VX, fade * get(VX) + buoy[...] * (along(SXX, 0) + along(SXY, 1) + z_x))
        send((VX, 0), (VX, 1))
        arrived((SXZ, 0), (SYZ, 1))
        put(VZ, fade * get(VZ) + buoy[...] * (along(SXZ, 0) + along(SYZ, 1) + z_z))
        send((VZ, 0), (VZ, 1))

        z_z = depth(VZ, False)
        z_x = depth(VX, True)
        z_y = depth(VY, True)
        sent(*stress_keys)
        arrived((VY, 0), (VX, 1))
        put(SXY, damp[...] * (get(SXY) + shear[...] * (along(VX, 1) + along(VY, 0))))

        @pl.when(t < steps - 1)
        def _():
            send((SXY, 0), (SXY, 1))

        arrived((VX, 0), (VY, 1))
        e_x, e_y, e_z = along(VX, 0), along(VY, 1), z_z
        base = lame[...] * (e_x + e_y + e_z) + push[t]
        twice = 2.0 * shear[...]
        n_x = damp[...] * (get(SXX) + (base + twice * e_x))
        n_y = damp[...] * (get(SYY) + (base + twice * e_y))
        n_z = damp[...] * (get(SZZ) + (base + twice * e_z))
        put(SXX, n_x)
        put(SYY, n_y)
        put(SZZ, n_z)
        press[...] = -(n_x + n_y + n_z) / 3.0

        @pl.when(t < steps - 1)
        def _():
            send((SXX, 0), (SYY, 1))

        arrived((VZ, 0), (VZ, 1))
        put(SXZ, damp[...] * (get(SXZ) + shear[...] * (z_x + along(VZ, 0))))
        put(SYZ, damp[...] * (get(SYZ) + shear[...] * (z_y + along(VZ, 1))))

        @pl.when(t < steps - 1)
        def _():
            send((SXZ, 0), (SYZ, 1))

        picked = jnp.dot(
            press[...].reshape(wx * wy, nz), probe_z[...],
            precision=EXACT, preferred_element_type=jnp.float32,
        )
        rows_y[0, pl.ds(t, 1), :] = jnp.sum(picked * probe_row[...], axis=0, keepdims=True)
        sent(*speed_keys)
        return carry

    lax.fori_loop(0, steps, step, 0)

    def gather(axis, buffer, ssem, rsem):
        n = extent[axis]
        copies = [
            pltpu.make_async_remote_copy(
                src_ref=buffer.at[0], dst_ref=buffer.at[d],
                send_sem=ssem.at[d], recv_sem=rsem.at[d],
                device_id={axis_name[axis]: lax.rem(place[axis] + d, n)},
                device_id_type=pl.DeviceIdType.MESH,
            )
            for d in range(1, n)
        ]
        for one in copies:
            one.start()
        return copies

    def total(buffer):
        value = buffer[0]
        for d in range(1, buffer.shape[0]):
            value = value + buffer[d]
        return value

    first = gather(1, rows_y, tsend_y, trecv_y)
    for f in (SXX, SYY, SZZ, SXY, SXZ, SYZ):
        out_ref[f] = get(f)
    for one in first:
        one.wait_recv()
    rows_x[0] = total(rows_y)
    second = gather(0, rows_x, tsend_x, trecv_x)
    for f in (VX, VY, VZ):
        out_ref[f] = damp[...] * get(f)
    for one in second:
        one.wait_recv()
    traces_ref[...] = total(rows_x)[:steps]
    for one in first + second:
        one.wait_send()


def body(nx, ny, wavefield, labels, lame, shear, density, source_cells, source_amps, receiver_cells):
    _, wx, wy, nz = wavefield.shape
    steps, sources = source_amps.shape
    probes = receiver_cells.shape[0]
    padded = -(-steps // 8) * 8
    cells = (wx, wy, nz)
    vmem = pl.BlockSpec(memory_space=pltpu.VMEM)
    smem = pl.BlockSpec(memory_space=pltpu.SMEM)
    anywhere = pl.BlockSpec(memory_space=pl.ANY)
    f32 = jnp.float32
    return pl.pallas_call(
        functools.partial(kernel, (nx, ny, steps)),
        out_shape=(
            jax.ShapeDtypeStruct(wavefield.shape, f32),
            jax.ShapeDtypeStruct((steps, probes), f32),
        ),
        in_specs=[anywhere, anywhere, smem, smem, smem, vmem, vmem, vmem],
        out_specs=(vmem, vmem),
        scratch_shapes=[
            pltpu.VMEM((9, wx + 2 * RIM_X, wy + 2 * RIM_Y, nz), f32),
            pltpu.VMEM(cells, jnp.int32),
            pltpu.VMEM(cells, f32),
            pltpu.VMEM(cells, f32),
            pltpu.VMEM(cells, f32),
            pltpu.VMEM(cells, f32),
            pltpu.VMEM((2, nz, nz), f32),
            pltpu.VMEM((nz, sources), f32),
            pltpu.VMEM((nz, probes), f32),
            pltpu.VMEM((wx * wy, probes), f32),
            pltpu.VMEM((steps,) + cells, f32),
            pltpu.VMEM(cells, f32),
            pltpu.VMEM((ny, padded, probes), f32),
            pltpu.VMEM((nx, padded, probes), f32),
            pltpu.SemaphoreType.DMA((10,)),
            pltpu.SemaphoreType.DMA((len(EXCHANGED), 2)),
            pltpu.SemaphoreType.DMA((len(EXCHANGED), 2)),
            pltpu.SemaphoreType.DMA((ny,)),
            pltpu.SemaphoreType.DMA((ny,)),
            pltpu.SemaphoreType.DMA((nx,)),
            pltpu.SemaphoreType.DMA((nx,)),
        ],
        compiler_params=pltpu.CompilerParams(
            collective_id=0, has_side_effects=True, vmem_limit_bytes=24 * 1024 * 1024
        ),
    )(
        wavefield, labels, lame, shear, density,
        source_cells.reshape(1, sources), source_amps, receiver_cells.reshape(1, probes),
    )


def solution(mesh):
    field = P(None, ("shot", "gx"), "gy", None)
    placed = (field, P("gx", "gy", None), P(), P(), P(), P("shot"), P(None, "shot"), P())
    return jax.shard_map(
        functools.partial(body, mesh.shape["gx"], mesh.shape["gy"]),
        mesh=mesh,
        in_specs=placed,
        out_specs=(field, P(None, "shot")),
        check_vma=False,
    )
```

```python
import functools

import jax
import jax.numpy as jnp
from jax import lax
from jax.experimental import pallas as pl
from jax.experimental.pallas import tpu as pltpu
from jax.sharding import PartitionSpec as P

coeffs = (1225.0 / 1024.0, -245.0 / 3072.0, 49.0 / 5120.0, -5.0 / 7168.0)
time_step = 0.15
sponge_width = 16.0

VX, VY, VZ, SXX, SYY, SZZ, SXY, SXZ, SYZ = range(9)
EXCHANGED = {
    (SXY, 0): False, (SXX, 0): True, (SXZ, 0): False,
    (SYY, 1): True, (SXY, 1): False, (SYZ, 1): False,
    (VY, 0): True, (VX, 0): False, (VZ, 0): True,
    (VX, 1): True, (VY, 1): False, (VZ, 1): True,
}
SLOT = {key: number for number, key in enumerate(EXCHANGED)}
RIM_X = 4
RIM_Y = 8
LIMIT = 24 * 1024 * 1024
EXACT = lax.Precision.HIGHEST


def quotient(value, count):
    if count & (count - 1) == 0:
        return lax.shift_right_logical(value, jnp.full(value.shape, count.bit_length() - 1, value.dtype))
    return lax.div(value, jnp.full(value.shape, count, value.dtype))


def remainder(value, count):
    if count & (count - 1) == 0:
        return value & (count - 1)
    return value - quotient(value, count) * count


def profile(position, count):
    distance = jnp.minimum(position, count - 1 - position).astype(jnp.float32)
    depth = jnp.maximum(sponge_width - distance, 0.0) / sponge_width
    return jnp.exp(-(0.5 * depth) * (0.5 * depth))


def kernel(
    sizes,
    wave_ref, labels_ref, lame_ref, shear_ref, density_ref,
    source_ref, amps_ref, probe_ref,
    out_ref, traces_ref,
    lame_table, shear_table, density_table, sources, amps, probes,
    F, labels, lame, shear, buoy, damp, bands, source_z, probe_z, probe_row, push, press,
    rows_y, rows_x,
    load_sem, send_sem, recv_sem, tsend_y, trecv_y, tsend_x, trecv_x,
):
    nx, ny, steps = sizes
    _, wx, wy, nz = wave_ref.shape
    gx, gy = lax.axis_index("gx"), lax.axis_index("gy")
    place = (gx, gy)
    extent = (nx, ny)
    axis_name = ("gx", "gy")
    LX, LY = slice(RIM_X, RIM_X + wx), slice(RIM_Y, RIM_Y + wy)

    def local(f):
        return F.at[f, LX, LY, :]

    loads = [
        pltpu.make_async_copy(wave_ref.at[f], local(f), load_sem.at[f]) for f in range(9)
    ]
    load_labels = pltpu.make_async_copy(labels_ref, labels, load_sem.at[9])
    small = [
        pltpu.make_async_copy(source, sink, load_sem.at[10 + number])
        for number, (source, sink) in enumerate((
            (lame_ref, lame_table), (shear_ref, shear_table), (density_ref, density_table),
            (source_ref, sources), (amps_ref, amps), (probe_ref, probes),
        ))
    ]
    for f in (SXY, SXX, SXZ, SYY, SYZ):
        loads[f].start()
    load_labels.start()
    for one in small:
        one.start()
    for f in (SZZ, VY, VX, VZ):
        loads[f].start()

    for f, axis in EXCHANGED:
        if axis == 0:
            F[f, :RIM_X, LY, :] = jnp.zeros((RIM_X, wy, nz), jnp.float32)
            F[f, RIM_X + wx :, LY, :] = jnp.zeros((RIM_X, wy, nz), jnp.float32)
        else:
            F[f, LX, :RIM_Y, :] = jnp.zeros((wx, RIM_Y, nz), jnp.float32)
            F[f, LX, RIM_Y + wy :, :] = jnp.zeros((wx, RIM_Y, nz), jnp.float32)
    rows_y[...] = jnp.zeros(rows_y.shape, jnp.float32)

    barrier = pltpu.get_barrier_semaphore()
    for axis in (0, 1):
        for d in range(1, extent[axis]):
            pl.semaphore_signal(
                barrier, inc=1,
                device_id={axis_name[axis]: lax.rem(place[axis] + d, extent[axis])},
                device_id_type=pl.DeviceIdType.MESH,
            )
    pl.semaphore_wait(barrier, nx + ny - 2)

    def copy(f, axis, up):
        forward = EXCHANGED[f, axis]
        n = extent[axis]
        target = lax.rem(place[axis] + (1 if up else n - 1), n)
        if axis == 0:
            count = 3 if forward == up else 4
            if up:
                src, dst = RIM_X + wx - count, RIM_X - count
            else:
                src, dst = RIM_X, RIM_X + wx
            source = F.at[f, src : src + count, LY, :]
            sink = F.at[f, dst : dst + count, LY, :]
        else:
            src, dst = (wy, 0) if up else (RIM_Y, RIM_Y + wy)
            source = F.at[f, LX, src : src + RIM_Y, :]
            sink = F.at[f, LX, dst : dst + RIM_Y, :]
        slot = SLOT[f, axis]
        return pltpu.make_async_remote_copy(
            src_ref=source, dst_ref=sink,
            send_sem=send_sem.at[slot, int(up)], recv_sem=recv_sem.at[slot, int(up)],
            device_id={axis_name[axis]: target}, device_id_type=pl.DeviceIdType.MESH,
        )

    has_low = (gx > 0, gy > 0)
    has_high = (gx < nx - 1, gy < ny - 1)

    def send(*keys):
        for f, axis in keys:
            @pl.when(has_high[axis])
            def _():
                copy(f, axis, True).start()

            @pl.when(has_low[axis])
            def _():
                copy(f, axis, False).start()

    def sent(*keys):
        for axis in (0, 1):
            mine = [f for f, a in keys if a == axis]

            @pl.when(has_high[axis])
            def _():
                for f in mine:
                    copy(f, axis, True).wait_send()

            @pl.when(has_low[axis])
            def _():
                for f in mine:
                    copy(f, axis, False).wait_send()

    def arrived(*keys):
        for f, axis in keys:
            @pl.when(has_low[axis])
            def _():
                copy(f, axis, True).wait_recv()

            @pl.when(has_high[axis])
            def _():
                copy(f, axis, False).wait_recv()

    def tap(f, axis, offset):
        if axis == 0:
            return F[f, RIM_X + offset : RIM_X + offset + wx, LY, :]
        return F[f, LX, RIM_Y + offset : RIM_Y + offset + wy, :]

    def along(f, axis):
        forward = EXCHANGED[f, axis]
        result = None
        for k in range(1, 5):
            later, earlier = (k, 1 - k) if forward else (k - 1, -k)
            term = coeffs[k - 1] * (tap(f, axis, later) - tap(f, axis, earlier))
            result = term if result is None else result + term
        return result

    def depth(f, forward):
        flat = F[f, LX, LY, :].reshape(wx * wy, nz)
        return jnp.dot(
            flat, bands[int(forward)], precision=EXACT, preferred_element_type=jnp.float32
        ).reshape(wx, wy, nz)

    stress_keys = [(SXY, 0), (SYY, 1), (SXX, 0), (SXY, 1), (SXZ, 0), (SYZ, 1)]
    speed_keys = [(VY, 0), (VX, 1), (VX, 0), (VY, 1), (VZ, 0), (VZ, 1)]

    for f in (SXY, SYY, SXX, SXZ, SYZ):
        loads[f].wait()
    send(*stress_keys)

    load_labels.wait()
    for one in small:
        one.wait()
    tissue = labels[...]

    def lookup(table):
        value = jnp.zeros(tissue.shape, jnp.float32)
        for number in range(table.shape[0]):
            value = jnp.where(tissue == number, table[number], value)
        return value

    lame[...] = time_step * lookup(lame_table)
    shear[...] = time_step * lookup(shear_table)
    buoy[...] = time_step / lookup(density_table)
    shape = (wx, wy, nz)
    damp[...] = (
        profile(gx * wx + lax.broadcasted_iota(jnp.int32, shape, 0), nx * wx)
        * profile(gy * wy + lax.broadcasted_iota(jnp.int32, shape, 1), ny * wy)
        * profile(lax.broadcasted_iota(jnp.int32, shape, 2), nz)
    )
    gap = lax.broadcasted_iota(jnp.int32, (nz, nz), 0) - lax.broadcasted_iota(
        jnp.int32, (nz, nz), 1
    )
    for forward in (0, 1):
        band = jnp.zeros((nz, nz), jnp.float32)
        for k in range(1, 5):
            later, earlier = (k, 1 - k) if forward else (k - 1, -k)
            band = jnp.where(gap == later, coeffs[k - 1], band)
            band = jnp.where(gap == earlier, -coeffs[k - 1], band)
        bands[forward] = band

    def locate(cells):
        cell_x = quotient(cells, ny * wy * nz)
        cell_y = remainder(quotient(cells, nz), ny * wy)
        near_x = cell_x - gx * wx
        near_y = cell_y - gy * wy
        inside = (near_x >= 0) & (near_x < wx) & (near_y >= 0) & (near_y < wy)
        return jnp.where(inside, near_x * wy + near_y, -1), remainder(cells, nz)

    def match(indices, count):
        wide = (count, indices.shape[1])
        return jnp.where(lax.broadcasted_iota(jnp.int32, wide, 0) == indices, 1.0, 0.0).astype(
            jnp.float32
        )

    row, deep = locate(sources[...])
    source_row = match(row, wx * wy)
    source_z[...] = match(deep, nz)
    row, deep = locate(probes[...])
    probe_row[...] = match(row, wx * wy)
    probe_z[...] = match(deep, nz)
    for t in range(steps):
        push[t] = lax.dot_general(
            source_row * (time_step * amps[t : t + 1, :]),
            source_z[...],
            (((1,), (1,)), ((), ())),
            precision=EXACT,
            preferred_element_type=jnp.float32,
        ).reshape(wx, wy, nz)

    for f in (SZZ, VY, VX, VZ):
        loads[f].wait()

    def put(f, value):
        F[f, LX, LY, :] = value

    def get(f):
        return F[f, LX, LY, :]

    def gather(axis, buffer, ssem, rsem):
        n = extent[axis]
        copies = [
            pltpu.make_async_remote_copy(
                src_ref=buffer.at[0], dst_ref=buffer.at[d],
                send_sem=ssem.at[d], recv_sem=rsem.at[d],
                device_id={axis_name[axis]: lax.rem(place[axis] + d, n)},
                device_id_type=pl.DeviceIdType.MESH,
            )
            for d in range(1, n)
        ]
        return copies

    def total(buffer):
        value = buffer[0]
        for d in range(1, buffer.shape[0]):
            value = value + buffer[d]
        return value

    first = gather(1, rows_y, tsend_y, trecv_y)
    second = gather(0, rows_x, tsend_x, trecv_x)

    def step(t, carry):
        fade = jnp.where(t == 0, 1.0, damp[...])
        z_y = depth(SYZ, False)
        z_x = depth(SXZ, False)
        z_z = depth(SZZ, True)
        arrived((SXY, 0), (SYY, 1))
        put(VY, fade * get(VY) + buoy[...] * (along(SXY, 0) + along(SYY, 1) + z_y))
        send((VY, 0), (VY, 1))
        arrived((SXX, 0), (SXY, 1))
        put(VX, fade * get(VX) + buoy[...] * (along(SXX, 0) + along(SXY, 1) + z_x))
        send((VX, 0), (VX, 1))
        arrived((SXZ, 0), (SYZ, 1))
        put(VZ, fade * get(VZ) + buoy[...] * (along(SXZ, 0) + along(SYZ, 1) + z_z))
        send((VZ, 0), (VZ, 1))

        z_z = depth(VZ, False)
        z_x = depth(VX, True)
        z_y = depth(VY, True)
        sent(*stress_keys)
        arrived((VY, 0), (VX, 1))
        put(SXY, damp[...] * (get(SXY) + shear[...] * (along(VX, 1) + along(VY, 0))))

        @pl.when(t < steps - 1)
        def _():
            send((SXY, 0), (SXY, 1))

        arrived((VX, 0), (VY, 1))
        e_x, e_y, e_z = along(VX, 0), along(VY, 1), z_z
        base = lame[...] * (e_x + e_y + e_z) + push[t]
        twice = 2.0 * shear[...]
        n_x = damp[...] * (get(SXX) + (base + twice * e_x))
        n_y = damp[...] * (get(SYY) + (base + twice * e_y))
        n_z = damp[...] * (get(SZZ) + (base + twice * e_z))
        put(SXX, n_x)
        put(SYY, n_y)
        put(SZZ, n_z)
        press[...] = -(n_x + n_y + n_z) / 3.0

        @pl.when(t < steps - 1)
        def _():
            send((SXX, 0), (SYY, 1))

        picked = jnp.dot(
            press[...].reshape(wx * wy, nz), probe_z[...],
            precision=EXACT, preferred_element_type=jnp.float32,
        )
        rows_y[0, pl.ds(t, 1), :] = jnp.sum(picked * probe_row[...], axis=0, keepdims=True)

        @pl.when(t == steps - 1)
        def _():
            for one in first:
                one.start()

        arrived((VZ, 0), (VZ, 1))
        put(SXZ, damp[...] * (get(SXZ) + shear[...] * (z_x + along(VZ, 0))))
        put(SYZ, damp[...] * (get(SYZ) + shear[...] * (z_y + along(VZ, 1))))

        @pl.when(t < steps - 1)
        def _():
            send((SXZ, 0), (SYZ, 1))

        sent(*speed_keys)
        return carry

    lax.fori_loop(0, steps, step, 0)

    stores = [
        pltpu.make_async_copy(local(f), out_ref.at[f], load_sem.at[f]) for f in range(9)
    ]
    for f in (SXX, SYY, SZZ, SXY, SXZ, SYZ):
        stores[f].start()
    for f in (VX, VY, VZ):
        put(f, damp[...] * get(f))
    for f in (VX, VY, VZ):
        stores[f].start()
    for one in first:
        one.wait_recv()
    rows_x[0] = total(rows_y)
    for one in second:
        one.start()
    for one in second:
        one.wait_recv()
    traces_ref[...] = total(rows_x)[:steps]
    for one in first + second:
        one.wait_send()
    for one in stores:
        one.wait()


def body(nx, ny, wavefield, labels, lame, shear, density, source_cells, source_amps, receiver_cells):
    _, wx, wy, nz = wavefield.shape
    steps, sources = source_amps.shape
    probes = receiver_cells.shape[0]
    padded = -(-steps // 8) * 8
    cells = (wx, wy, nz)
    vmem = pl.BlockSpec(memory_space=pltpu.VMEM)
    f32 = jnp.float32
    return pl.pallas_call(
        functools.partial(kernel, (nx, ny, steps)),
        out_shape=(
            jax.ShapeDtypeStruct(wavefield.shape, f32),
            jax.ShapeDtypeStruct((steps, probes), f32),
        ),
        in_specs=[pl.BlockSpec(memory_space=pltpu.HBM)] * 8,
        out_specs=(vmem, vmem),
        scratch_shapes=[
            pltpu.SMEM(lame.shape, f32),
            pltpu.SMEM(shear.shape, f32),
            pltpu.SMEM(density.shape, f32),
            pltpu.VMEM((1, sources), jnp.int32),
            pltpu.VMEM((steps, sources), f32),
            pltpu.VMEM((1, probes), jnp.int32),
            pltpu.VMEM((9, wx + 2 * RIM_X, wy + 2 * RIM_Y, nz), f32),
            pltpu.VMEM(cells, jnp.int32),
            pltpu.VMEM(cells, f32),
            pltpu.VMEM(cells, f32),
            pltpu.VMEM(cells, f32),
            pltpu.VMEM(cells, f32),
            pltpu.VMEM((2, nz, nz), f32),
            pltpu.VMEM((nz, sources), f32),
            pltpu.VMEM((nz, probes), f32),
            pltpu.VMEM((wx * wy, probes), f32),
            pltpu.VMEM((steps,) + cells, f32),
            pltpu.VMEM(cells, f32),
            pltpu.VMEM((ny, padded, probes), f32),
            pltpu.VMEM((nx, padded, probes), f32),
            pltpu.SemaphoreType.DMA((16,)),
            pltpu.SemaphoreType.DMA((len(EXCHANGED), 2)),
            pltpu.SemaphoreType.DMA((len(EXCHANGED), 2)),
            pltpu.SemaphoreType.DMA((ny,)),
            pltpu.SemaphoreType.DMA((ny,)),
            pltpu.SemaphoreType.DMA((nx,)),
            pltpu.SemaphoreType.DMA((nx,)),
        ],
        compiler_params=pltpu.CompilerParams(
            collective_id=0, has_side_effects=True, vmem_limit_bytes=LIMIT
        ),
    )(
        *(
            pltpu.with_memory_space_constraint(value, pltpu.HBM)
            for value in (
                wavefield, labels, lame, shear, density,
                source_cells.reshape(1, sources), source_amps, receiver_cells.reshape(1, probes),
            )
        )
    )


def solution(mesh):
    field = P(None, ("shot", "gx"), "gy", None)
    placed = (field, P("gx", "gy", None), P(), P(), P(), P("shot"), P(None, "shot"), P())
    return jax.shard_map(
        functools.partial(body, mesh.shape["gx"], mesh.shape["gy"]),
        mesh=mesh,
        in_specs=placed,
        out_specs=(field, P(None, "shot")),
        check_vma=False,
    )
```

```python
import functools

import jax
import jax.numpy as jnp
from jax import lax
from jax.experimental import pallas as pl
from jax.experimental.pallas import tpu as pltpu
from jax.sharding import PartitionSpec as P

coeffs = (1225.0 / 1024.0, -245.0 / 3072.0, 49.0 / 5120.0, -5.0 / 7168.0)
time_step = 0.15
sponge_width = 16.0

VX, VY, VZ, SXX, SYY, SZZ, SXY, SXZ, SYZ = range(9)
EXCHANGED = {
    (SXY, 0): False, (SXX, 0): True, (SXZ, 0): False,
    (SYY, 1): True, (SXY, 1): False, (SYZ, 1): False,
    (VY, 0): True, (VX, 0): False, (VZ, 0): True,
    (VX, 1): True, (VY, 1): False, (VZ, 1): True,
}
SLOT = {key: number for number, key in enumerate(EXCHANGED)}
RIM_X = 4
RIM_Y = 8
LIMIT = 24 * 1024 * 1024
EXACT = lax.Precision.HIGHEST


def quotient(value, count):
    if count & (count - 1) == 0:
        return lax.shift_right_logical(value, jnp.full(value.shape, count.bit_length() - 1, value.dtype))
    return lax.div(value, jnp.full(value.shape, count, value.dtype))


def remainder(value, count):
    if count & (count - 1) == 0:
        return value & (count - 1)
    return value - quotient(value, count) * count


def profile(position, count):
    distance = jnp.minimum(position, count - 1 - position).astype(jnp.float32)
    depth = jnp.maximum(sponge_width - distance, 0.0) / sponge_width
    return jnp.exp(-(0.5 * depth) * (0.5 * depth))


def kernel(
    sizes,
    wave_ref, labels_ref, lame_ref, shear_ref, density_ref,
    source_ref, amps_ref, probe_ref,
    out_ref, traces_ref,
    lame_table, shear_table, density_table, sources, amps, probes,
    F, labels, lame, shear, buoy, damp, bands, source_z, probe_z, probe_row, push, press,
    rows_y, rows_x, last, lsend, lrecv,
    load_sem, send_sem, recv_sem, tsend_y, trecv_y, tsend_x, trecv_x,
):
    nx, ny, steps = sizes
    _, wx, wy, nz = wave_ref.shape
    gx, gy = lax.axis_index("gx"), lax.axis_index("gy")
    place = (gx, gy)
    extent = (nx, ny)
    axis_name = ("gx", "gy")
    LX, LY = slice(RIM_X, RIM_X + wx), slice(RIM_Y, RIM_Y + wy)

    def local(f):
        return F.at[f, LX, LY, :]

    loads = [
        pltpu.make_async_copy(wave_ref.at[f], local(f), load_sem.at[f]) for f in range(9)
    ]
    load_labels = pltpu.make_async_copy(labels_ref, labels, load_sem.at[9])
    small = [
        pltpu.make_async_copy(source, sink, load_sem.at[10 + number])
        for number, (source, sink) in enumerate((
            (lame_ref, lame_table), (shear_ref, shear_table), (density_ref, density_table),
            (source_ref, sources), (amps_ref, amps), (probe_ref, probes),
        ))
    ]
    for f in (SXY, SXX, SXZ, SYY, SYZ):
        loads[f].start()
    load_labels.start()
    for one in small:
        one.start()
    for f in (SZZ, VY, VX, VZ):
        loads[f].start()

    for f, axis in EXCHANGED:
        if axis == 0:
            F[f, :RIM_X, LY, :] = jnp.zeros((RIM_X, wy, nz), jnp.float32)
            F[f, RIM_X + wx :, LY, :] = jnp.zeros((RIM_X, wy, nz), jnp.float32)
        else:
            F[f, LX, :RIM_Y, :] = jnp.zeros((wx, RIM_Y, nz), jnp.float32)
            F[f, LX, RIM_Y + wy :, :] = jnp.zeros((wx, RIM_Y, nz), jnp.float32)
    rows_y[...] = jnp.zeros(rows_y.shape, jnp.float32)

    barrier = pltpu.get_barrier_semaphore()
    peers = [(a, b) for a in range(nx) for b in range(ny) if a + b > 0]

    def peer(a, b):
        return {"gx": lax.rem(gx + a, nx), "gy": lax.rem(gy + b, ny)}

    for a, b in peers:
        pl.semaphore_signal(
            barrier, inc=1, device_id=peer(a, b), device_id_type=pl.DeviceIdType.MESH
        )
    pl.semaphore_wait(barrier, len(peers))

    def copy(f, axis, up):
        forward = EXCHANGED[f, axis]
        n = extent[axis]
        target = lax.rem(place[axis] + (1 if up else n - 1), n)
        if axis == 0:
            count = 3 if forward == up else 4
            if up:
                src, dst = RIM_X + wx - count, RIM_X - count
            else:
                src, dst = RIM_X, RIM_X + wx
            source = F.at[f, src : src + count, LY, :]
            sink = F.at[f, dst : dst + count, LY, :]
        else:
            src, dst = (wy, 0) if up else (RIM_Y, RIM_Y + wy)
            source = F.at[f, LX, src : src + RIM_Y, :]
            sink = F.at[f, LX, dst : dst + RIM_Y, :]
        slot = SLOT[f, axis]
        return pltpu.make_async_remote_copy(
            src_ref=source, dst_ref=sink,
            send_sem=send_sem.at[slot, int(up)], recv_sem=recv_sem.at[slot, int(up)],
            device_id={axis_name[axis]: target}, device_id_type=pl.DeviceIdType.MESH,
        )

    has_low = (gx > 0, gy > 0)
    has_high = (gx < nx - 1, gy < ny - 1)

    def send(*keys):
        for f, axis in keys:
            @pl.when(has_high[axis])
            def _():
                copy(f, axis, True).start()

            @pl.when(has_low[axis])
            def _():
                copy(f, axis, False).start()

    def sent(*keys):
        for axis in (0, 1):
            mine = [f for f, a in keys if a == axis]

            @pl.when(has_high[axis])
            def _():
                for f in mine:
                    copy(f, axis, True).wait_send()

            @pl.when(has_low[axis])
            def _():
                for f in mine:
                    copy(f, axis, False).wait_send()

    def arrived(*keys):
        for f, axis in keys:
            @pl.when(has_low[axis])
            def _():
                copy(f, axis, True).wait_recv()

            @pl.when(has_high[axis])
            def _():
                copy(f, axis, False).wait_recv()

    def tap(f, axis, offset):
        if axis == 0:
            return F[f, RIM_X + offset : RIM_X + offset + wx, LY, :]
        return F[f, LX, RIM_Y + offset : RIM_Y + offset + wy, :]

    def along(f, axis):
        forward = EXCHANGED[f, axis]
        result = None
        for k in range(1, 5):
            later, earlier = (k, 1 - k) if forward else (k - 1, -k)
            term = coeffs[k - 1] * (tap(f, axis, later) - tap(f, axis, earlier))
            result = term if result is None else result + term
        return result

    def depth(f, forward):
        flat = F[f, LX, LY, :].reshape(wx * wy, nz)
        return jnp.dot(
            flat, bands[int(forward)], precision=EXACT, preferred_element_type=jnp.float32
        ).reshape(wx, wy, nz)

    stress_keys = [(SXY, 0), (SYY, 1), (SXX, 0), (SXY, 1), (SXZ, 0), (SYZ, 1)]
    speed_keys = [(VY, 0), (VX, 1), (VX, 0), (VY, 1), (VZ, 0), (VZ, 1)]

    for f in (SXY, SYY, SXX, SXZ, SYZ):
        loads[f].wait()
    send(*stress_keys)

    load_labels.wait()
    for one in small:
        one.wait()
    tissue = labels[...]

    def lookup(table):
        value = jnp.zeros(tissue.shape, jnp.float32)
        for number in range(table.shape[0]):
            value = jnp.where(tissue == number, table[number], value)
        return value

    lame[...] = time_step * lookup(lame_table)
    shear[...] = time_step * lookup(shear_table)
    buoy[...] = time_step / lookup(density_table)
    shape = (wx, wy, nz)
    damp[...] = (
        profile(gx * wx + lax.broadcasted_iota(jnp.int32, shape, 0), nx * wx)
        * profile(gy * wy + lax.broadcasted_iota(jnp.int32, shape, 1), ny * wy)
        * profile(lax.broadcasted_iota(jnp.int32, shape, 2), nz)
    )
    gap = lax.broadcasted_iota(jnp.int32, (nz, nz), 0) - lax.broadcasted_iota(
        jnp.int32, (nz, nz), 1
    )
    for forward in (0, 1):
        band = jnp.zeros((nz, nz), jnp.float32)
        for k in range(1, 5):
            later, earlier = (k, 1 - k) if forward else (k - 1, -k)
            band = jnp.where(gap == later, coeffs[k - 1], band)
            band = jnp.where(gap == earlier, -coeffs[k - 1], band)
        bands[forward] = band

    def locate(cells):
        cell_x = quotient(cells, ny * wy * nz)
        cell_y = remainder(quotient(cells, nz), ny * wy)
        near_x = cell_x - gx * wx
        near_y = cell_y - gy * wy
        inside = (near_x >= 0) & (near_x < wx) & (near_y >= 0) & (near_y < wy)
        return jnp.where(inside, near_x * wy + near_y, -1), remainder(cells, nz)

    def match(indices, count):
        wide = (count, indices.shape[1])
        return jnp.where(lax.broadcasted_iota(jnp.int32, wide, 0) == indices, 1.0, 0.0).astype(
            jnp.float32
        )

    row, deep = locate(sources[...])
    source_row = match(row, wx * wy)
    source_z[...] = match(deep, nz)
    row, deep = locate(probes[...])
    probe_row[...] = match(row, wx * wy)
    probe_z[...] = match(deep, nz)
    for t in range(steps):
        push[t] = lax.dot_general(
            source_row * (time_step * amps[t : t + 1, :]),
            source_z[...],
            (((1,), (1,)), ((), ())),
            precision=EXACT,
            preferred_element_type=jnp.float32,
        ).reshape(wx, wy, nz)

    for f in (SZZ, VY, VX, VZ):
        loads[f].wait()

    def put(f, value):
        F[f, LX, LY, :] = value

    def get(f):
        return F[f, LX, LY, :]

    def gather(axis, buffer, ssem, rsem):
        n = extent[axis]
        copies = [
            pltpu.make_async_remote_copy(
                src_ref=buffer.at[0], dst_ref=buffer.at[d],
                send_sem=ssem.at[d], recv_sem=rsem.at[d],
                device_id={axis_name[axis]: lax.rem(place[axis] + d, n)},
                device_id_type=pl.DeviceIdType.MESH,
            )
            for d in range(1, n)
        ]
        return copies

    def total(buffer):
        value = buffer[0]
        for d in range(1, buffer.shape[0]):
            value = value + buffer[d]
        return value

    spread = [
        pltpu.make_async_remote_copy(
            src_ref=last.at[0], dst_ref=last.at[a * ny + b],
            send_sem=lsend.at[a * ny + b], recv_sem=lrecv.at[a * ny + b],
            device_id=peer(a, b), device_id_type=pl.DeviceIdType.MESH,
        )
        for a, b in peers
    ]
    first = gather(1, rows_y, tsend_y, trecv_y)
    second = gather(0, rows_x, tsend_x, trecv_x)

    def step(t, carry):
        fade = jnp.where(t == 0, 1.0, damp[...])
        z_y = depth(SYZ, False)
        z_x = depth(SXZ, False)
        z_z = depth(SZZ, True)
        arrived((SXY, 0), (SYY, 1))
        put(VY, fade * get(VY) + buoy[...] * (along(SXY, 0) + along(SYY, 1) + z_y))
        send((VY, 0), (VY, 1))
        arrived((SXX, 0), (SXY, 1))
        put(VX, fade * get(VX) + buoy[...] * (along(SXX, 0) + along(SXY, 1) + z_x))
        send((VX, 0), (VX, 1))
        arrived((SXZ, 0), (SYZ, 1))
        put(VZ, fade * get(VZ) + buoy[...] * (along(SXZ, 0) + along(SYZ, 1) + z_z))
        send((VZ, 0), (VZ, 1))

        @pl.when(t == steps - 1)
        def _():
            for one in first:
                one.wait_recv()
            rows_x[0] = total(rows_y)
            for one in second:
                one.start()

        z_z = depth(VZ, False)
        z_x = depth(VX, True)
        z_y = depth(VY, True)
        sent(*stress_keys)
        arrived((VY, 0), (VX, 1))
        put(SXY, damp[...] * (get(SXY) + shear[...] * (along(VX, 1) + along(VY, 0))))

        @pl.when(t < steps - 1)
        def _():
            send((SXY, 0), (SXY, 1))

        arrived((VX, 0), (VY, 1))
        e_x, e_y, e_z = along(VX, 0), along(VY, 1), z_z
        base = lame[...] * (e_x + e_y + e_z) + push[t]
        twice = 2.0 * shear[...]
        n_x = damp[...] * (get(SXX) + (base + twice * e_x))
        n_y = damp[...] * (get(SYY) + (base + twice * e_y))
        n_z = damp[...] * (get(SZZ) + (base + twice * e_z))
        put(SXX, n_x)
        put(SYY, n_y)
        put(SZZ, n_z)
        press[...] = -(n_x + n_y + n_z) / 3.0

        @pl.when(t < steps - 1)
        def _():
            send((SXX, 0), (SYY, 1))

        picked = jnp.dot(
            press[...].reshape(wx * wy, nz), probe_z[...],
            precision=EXACT, preferred_element_type=jnp.float32,
        )
        line = jnp.sum(picked * probe_row[...], axis=0, keepdims=True)

        @pl.when(t < steps - 1)
        def _():
            rows_y[0, pl.ds(t, 1), :] = line

        @pl.when(t == steps - 1)
        def _():
            last[0] = line
            for one in spread:
                one.start()

        arrived((VZ, 0), (VZ, 1))
        put(SXZ, damp[...] * (get(SXZ) + shear[...] * (z_x + along(VZ, 0))))
        put(SYZ, damp[...] * (get(SYZ) + shear[...] * (z_y + along(VZ, 1))))

        @pl.when(t < steps - 1)
        def _():
            send((SXZ, 0), (SYZ, 1))

        @pl.when(t == steps - 2)
        def _():
            for one in first:
                one.start()

        sent(*speed_keys)
        return carry

    lax.fori_loop(0, steps, step, 0)

    stores = [
        pltpu.make_async_copy(local(f), out_ref.at[f], load_sem.at[f]) for f in range(9)
    ]
    for f in (SXX, SYY, SZZ, SXY, SXZ, SYZ):
        stores[f].start()
    for f in (VX, VY, VZ):
        put(f, damp[...] * get(f))
    for f in (VX, VY, VZ):
        stores[f].start()
    for one in second:
        one.wait_recv()
    for one in spread:
        one.wait_recv()
    traces_ref[...] = total(rows_x)[:steps]
    traces_ref[steps - 1 : steps, :] = total(last)
    for one in first + second + spread:
        one.wait_send()
    for one in stores:
        one.wait()


def body(nx, ny, wavefield, labels, lame, shear, density, source_cells, source_amps, receiver_cells):
    _, wx, wy, nz = wavefield.shape
    steps, sources = source_amps.shape
    probes = receiver_cells.shape[0]
    padded = -(-steps // 8) * 8
    cells = (wx, wy, nz)
    vmem = pl.BlockSpec(memory_space=pltpu.VMEM)
    f32 = jnp.float32
    return pl.pallas_call(
        functools.partial(kernel, (nx, ny, steps)),
        out_shape=(
            jax.ShapeDtypeStruct(wavefield.shape, f32),
            jax.ShapeDtypeStruct((steps, probes), f32),
        ),
        in_specs=[pl.BlockSpec(memory_space=pltpu.HBM)] * 8,
        out_specs=(vmem, vmem),
        scratch_shapes=[
            pltpu.SMEM(lame.shape, f32),
            pltpu.SMEM(shear.shape, f32),
            pltpu.SMEM(density.shape, f32),
            pltpu.VMEM((1, sources), jnp.int32),
            pltpu.VMEM((steps, sources), f32),
            pltpu.VMEM((1, probes), jnp.int32),
            pltpu.VMEM((9, wx + 2 * RIM_X, wy + 2 * RIM_Y, nz), f32),
            pltpu.VMEM(cells, jnp.int32),
            pltpu.VMEM(cells, f32),
            pltpu.VMEM(cells, f32),
            pltpu.VMEM(cells, f32),
            pltpu.VMEM(cells, f32),
            pltpu.VMEM((2, nz, nz), f32),
            pltpu.VMEM((nz, sources), f32),
            pltpu.VMEM((nz, probes), f32),
            pltpu.VMEM((wx * wy, probes), f32),
            pltpu.VMEM((steps,) + cells, f32),
            pltpu.VMEM(cells, f32),
            pltpu.VMEM((ny, padded, probes), f32),
            pltpu.VMEM((nx, padded, probes), f32),
            pltpu.VMEM((nx * ny, 1, probes), f32),
            pltpu.SemaphoreType.DMA((nx * ny,)),
            pltpu.SemaphoreType.DMA((nx * ny,)),
            pltpu.SemaphoreType.DMA((16,)),
            pltpu.SemaphoreType.DMA((len(EXCHANGED), 2)),
            pltpu.SemaphoreType.DMA((len(EXCHANGED), 2)),
            pltpu.SemaphoreType.DMA((ny,)),
            pltpu.SemaphoreType.DMA((ny,)),
            pltpu.SemaphoreType.DMA((nx,)),
            pltpu.SemaphoreType.DMA((nx,)),
        ],
        compiler_params=pltpu.CompilerParams(
            collective_id=0, has_side_effects=True, vmem_limit_bytes=LIMIT
        ),
    )(
        *(
            pltpu.with_memory_space_constraint(value, pltpu.HBM)
            for value in (
                wavefield, labels, lame, shear, density,
                source_cells.reshape(1, sources), source_amps, receiver_cells.reshape(1, probes),
            )
        )
    )


def solution(mesh):
    field = P(None, ("shot", "gx"), "gy", None)
    placed = (field, P("gx", "gy", None), P(), P(), P(), P("shot"), P(None, "shot"), P())
    return jax.shard_map(
        functools.partial(body, mesh.shape["gx"], mesh.shape["gy"]),
        mesh=mesh,
        in_specs=placed,
        out_specs=(field, P(None, "shot")),
        check_vma=False,
    )
```
